16 devices in a mesh: dp: 2 (over y, z), dcp: 8 (over x, core).
Axes of the slice: x: 4, y: 2, z: 1, core: 2. Of those that a mesh axis runs over, the one named last changes fastest.
The devices are a block of a 4x4x8 slice.
Arguments:
- q: bfloat16 [256, 16, 576], P('dp', 'dcp'), parts along dimension 0
- cache: bfloat16 [256, 32, 8, 8, 576], P('dp', None, 'dcp'), parts along dimension 0
- lens: int32 [256], P('dp'), parts along dimension 0
Outputs:
- output: bfloat16 [256, 16, 512], P('dp', 'dcp'), parts along dimension 0
There are 2 independent parts. The reference program is written for one: setup_inputs(seed, part) draws one part's arguments, and reference() takes and returns one part's arrays. A program takes and returns all parts, laid end to end along the dimension named above; each array names one.
All inputs are finite; a program needn't handle non-finite values.
Results may differ from the reference program's by a relative error of at most 0.0081033.
Values are sent between devices in bfloat16 or wider.
A program may use at most 768 MiB of HBM per device.

```python
import jax
import jax.numpy as jnp
from jax import lax

B = 128
S = 2048
PAGE = 8
DCP = 8
HEADS = 16
LORA = 512
ROPE = 64
NOPE = 128

R = S // (PAGE * DCP)
K = LORA + ROPE


def setup_inputs(seed: int = 0, part: int = 0) -> dict:
    key = jax.random.fold_in(jax.random.key(seed), part)
    kq, kc, kl = jax.random.split(key, 3)
    qs = 1.5 * ((NOPE + ROPE) / 2.0) ** 0.5
    scale = jnp.concatenate([jnp.full((LORA,), qs / LORA ** 0.5, jnp.float32), jnp.full((ROPE,), qs / ROPE ** 0.5, jnp.float32)])
    q = (jax.random.normal(kq, (B, HEADS, K), jnp.float32) * scale).astype(jnp.bfloat16)
    cache = jax.random.normal(kc, (B, R, DCP, PAGE, K), jnp.float32).astype(jnp.bfloat16)
    lens = jax.random.randint(kl, (B,), S // 4, S + 1, jnp.int32)
    return {'q': q, 'cache': cache, 'lens': lens}


def reference(q, cache, lens):
    c = cache.reshape(B, S, K)
    pos = jnp.arange(S)

    def one(args):
        qb, cb, lb = args
        s = jnp.dot(qb, cb.T, preferred_element_type=jnp.float32) / (NOPE + ROPE) ** 0.5
        s = jnp.where(pos[None, :] < lb, s, -jnp.inf)
        a = jax.nn.softmax(s, axis=1)
        o = jnp.dot(a, cb[:, :LORA].astype(jnp.float32), preferred_element_type=jnp.float32)
        return o.astype(jnp.bfloat16)

    return lax.map(one, (q, c, lens))
```

```python
import functools
import jax
import jax.numpy as jnp
from jax import lax
from jax.experimental import pallas as pl
from jax.experimental.pallas import tpu as pltpu
from jax.sharding import PartitionSpec as P

ROPE = 64
QK_DIM = 192
SCALE = QK_DIM ** -0.5
LOG2E = 1.4426950408889634
KP = 640
TB = 64


def kernel(n, lm_ref, q_ref, c_hbm, o_ref, lse_ref, stage, y, qt, s_ref, sems):
    d = lax.axis_index('dcp')
    nr, page, k, b = c_hbm.shape
    g = y.shape[1]
    t = nr * page
    lora = k - ROPE

    def fetch(r, slot):
        return pltpu.make_async_copy(c_hbm.at[r], stage.at[slot], sems.at[slot])

    for i in range(2):
        fetch(i, i).start()

    def load(r, _):
        slot = lax.rem(r, 3)

        @pl.when(r + 2 < nr)
        def _():
            fetch(r + 2, lax.rem(r + 2, 3)).start()

        fetch(r, slot).wait()
        for p in range(page):
            x = stage[slot, p]
            xt = jnp.concatenate([x, jnp.zeros((KP - k, b), x.dtype)], 0).T
            y[r * page + p] = xt.reshape(g, b // g, KP)
        return 0

    lax.fori_loop(0, nr, load, 0)

    tl = lax.broadcasted_iota(jnp.int32, (TB, 1, 1), 0)

    def group(gi, _):
        qt[...] = q_ref[gi].T

        def qk(j, m):
            lhs = y[pl.ds(j * TB, TB), gi].reshape(TB * 16, KP)
            s = jnp.dot(lhs, qt[...], preferred_element_type=jnp.float32)
            s = s.reshape(TB, 2, 8, 256)
            ti = tl + j * TB
            pos = ((ti // page) * n + d) * page + lax.rem(ti, page)
            out = []
            for o in range(2):
                so = s[:, o, :, o * 128:(o + 1) * 128] * (SCALE * LOG2E)
                so = jnp.where(pos < lm_ref[gi, o][None], so, -jnp.inf)
                s_ref[o, pl.ds(j * TB, TB)] = so
                out.append(jnp.maximum(m[o], jnp.max(so, axis=0)))
            return tuple(out)

        m = lax.fori_loop(0, t // TB, qk, (jnp.full((8, 128), -jnp.inf, jnp.float32),) * 2)
        m = [jnp.max(x, axis=0, keepdims=True) for x in m]
        m = [jnp.where(x == -jnp.inf, 0.0, x) for x in m]
        lane = lax.broadcasted_iota(jnp.int32, (128, TB * 16), 1)
        first = lax.rem(lane, 16) < 8

        def pv(j, carry):
            l, acc = carry
            ps = []
            ls = []
            for o in range(2):
                p = jnp.exp2(s_ref[o, pl.ds(j * TB, TB)] - m[o][None])
                ls.append(l[o] + jnp.sum(p, axis=0))
                ps.append(p)
            pm = jnp.concatenate(ps, axis=1).astype(jnp.bfloat16).reshape(TB * 16, 128).T
            z = jnp.zeros_like(pm)
            pt = jnp.concatenate([jnp.where(first, pm, z), jnp.where(first, z, pm)], axis=0)
            v = y[pl.ds(j * TB, TB), gi, :, 0:lora].reshape(TB * 16, lora)
            acc = acc + jnp.dot(pt, v, preferred_element_type=jnp.float32)
            return tuple(ls), acc

        l, acc = lax.fori_loop(0, t // TB, pv, ((jnp.zeros((8, 128), jnp.float32),) * 2, jnp.zeros((256, lora), jnp.float32)))
        for o in range(2):
            lo = jnp.sum(l[o], axis=0, keepdims=True)
            has = lo > 0.0
            lsafe = jnp.where(has, lo, 1.0)
            lse_ref[gi, o:o + 1] = jnp.where(has, m[o] + jnp.log2(lsafe), -jnp.inf)
            col = jnp.broadcast_to(1.0 / lsafe, (8, 128)).T[:, 0:1]
            o_ref[gi, o] = (acc[o * 128:(o + 1) * 128] * col).astype(jnp.bfloat16)
        return 0

    lax.fori_loop(0, g, group, 0)


def solution(mesh):
    n = mesh.shape['dcp']

    def local(q, cache, lens):
        b, hl, k = q.shape
        nr, page = cache.shape[1], cache.shape[3]
        lora = k - ROPE
        g = b // 16
        h = n * hl
        qa = lax.all_gather(q, 'dcp', axis=0)
        qa = jnp.pad(qa.reshape(n, g, 2, 8, hl, k), [(0, 0)] * 5 + [(0, KP - k)])
        qa = qa.transpose(1, 2, 0, 3, 4, 5).reshape(g, 256, KP)
        lane = jnp.arange(128)
        diag = (lane[None, :] // hl) % 8 == jnp.arange(8)[:, None]
        lm = jnp.where(diag, lens.reshape(g, 2, 8)[:, :, :, None], 0)
        ct = jnp.transpose(cache, (1, 2, 3, 4, 0)).reshape(nr, page, k, b)
        part, lse = pl.pallas_call(
            functools.partial(kernel, n),
            out_shape=(jax.ShapeDtypeStruct((g, 2, 128, lora), jnp.bfloat16), jax.ShapeDtypeStruct((g, 2, 128), jnp.float32)),
            in_specs=[pl.BlockSpec(memory_space=pltpu.VMEM)] * 2 + [pl.BlockSpec(memory_space=pl.ANY)],
            out_specs=(pl.BlockSpec(memory_space=pltpu.VMEM),) * 2,
            scratch_shapes=[
                pltpu.VMEM((3, page, k, b), jnp.bfloat16),
                pltpu.VMEM((nr * page, g, 16, KP), jnp.bfloat16),
                pltpu.VMEM((KP, 256), jnp.bfloat16),
                pltpu.VMEM((2, nr * page, 8, 128), jnp.float32),
                pltpu.SemaphoreType.DMA((3,)),
            ],
            compiler_params=pltpu.CompilerParams(vmem_limit_bytes=67043328),
        )(lm, qa, ct)
        od = lax.all_to_all(part.reshape(g, 2, n, 16, lora), 'dcp', 2, 2, tiled=True)
        le = lax.all_to_all(lse.reshape(g, 2, n, 16), 'dcp', 2, 2, tiled=True)
        top = jnp.max(le, axis=2, keepdims=True)
        w = jnp.exp2(le - top)
        o = jnp.sum(w[..., None] * od.astype(jnp.float32), axis=2) / jnp.sum(w, axis=2)[..., None]
        return o.astype(jnp.bfloat16).reshape(b, hl, lora)

    return jax.shard_map(local, mesh=mesh, in_specs=(P('dp', 'dcp', None), P('dp', None, 'dcp', None, None), P('dp')), out_specs=P('dp', 'dcp', None), check_vma=False)
```

```python
import functools
import jax
import jax.numpy as jnp
from jax import lax
from jax.experimental import pallas as pl
from jax.experimental.pallas import tpu as pltpu
from jax.sharding import PartitionSpec as P

ROPE = 64
QK_DIM = 192
SCALE = QK_DIM ** -0.5
LOG2E = 1.4426950408889634
KP = 640
TQ = 64
TV = 64
MESH = pl.DeviceIdType.MESH


def kernel(lm_ref, q_ref, c_hbm, o_ref, y, qall, qt, s0_ref, s1_ref, accs, arecv, part, precv, lses, lrecv, cols,
           csem, qs, qr, ss, sr, ps, pr, ls, lr):
    me = lax.axis_index('dcp')
    dp = lax.axis_index('dp')
    x, c = me // 2, lax.rem(me, 2)
    nx = 4
    n = 2 * nx
    nr, page, k, b = c_hbm.shape
    g = b // 16
    t = nr * page
    lora = k - ROPE

    def at(dx, same):
        xx = lax.rem(x + dx + nx, nx)
        return (dp, xx * 2 + (c if same else 1 - c))

    def slot(dx):
        return c * nx + lax.rem(x + dx + nx, nx)

    def pslot(dx):
        return (1 - c) * nx + lax.rem(x + dx + nx, nx)

    def fetch(r):
        return pltpu.make_async_copy(c_hbm.at[r], y.at[pl.ds(r * page, page), 0:k], csem.at[r])

    for r in range(nr):
        fetch(r).start()

    barrier = pltpu.get_barrier_semaphore()
    for dev in (at(1, True), at(-1, True), at(2, True), at(0, False)):
        pl.semaphore_signal(barrier, inc=1, device_id=dev, device_id_type=MESH)
    pl.semaphore_wait(barrier, 4)

    def rc(src, dst, s, r, dev):
        return pltpu.make_async_remote_copy(src_ref=src, dst_ref=dst, send_sem=s, recv_sem=r, device_id=dev, device_id_type=MESH)

    def qsend(gi, kind):
        sl = {0: slot(0), 1: slot(0), 2: slot(0), 3: slot(-1), 4: slot(-1), 5: slot(1), 6: slot(1), 7: slot(2)}[kind]
        dev = {0: at(1, True), 1: at(-1, True), 4: at(1, True), 6: at(-1, True)}.get(kind, at(0, False))
        half = {4: 0, 6: 1}.get(kind)
        if kind <= 2:
            src, dst = q_ref.at[gi], qall.at[gi, sl]
        elif half is None:
            src = dst = qall.at[gi, sl]
        else:
            src = dst = qall.at[gi, sl, half]
        return rc(src, dst, qs.at[gi, kind], qr.at[gi, kind], dev)

    def qwait(gi, kind):
        sl = {0: slot(-1), 1: slot(1), 2: pslot(0), 3: pslot(-1), 4: slot(2), 5: pslot(1), 6: slot(2), 7: pslot(2)}[kind]
        half = {4: 0, 6: 1}.get(kind)
        ref = qall.at[gi, sl] if half is None else qall.at[gi, sl, half]
        rc(ref, ref, qs.at[gi, kind], qr.at[gi, kind], at(0, False)).wait_recv()

    for gi in range(g):
        for kind in range(3):
            qsend(gi, kind).start()
        qall[gi, slot(0)] = q_ref[gi]

    def relay1(gi):
        qwait(gi, 0)
        qsend(gi, 4).start()
        qsend(gi, 3).start()
        qwait(gi, 1)
        qsend(gi, 6).start()
        qsend(gi, 5).start()

    def relay2(gi):
        qwait(gi, 4)
        qwait(gi, 6)
        qsend(gi, 7).start()

    def load(r, _):
        fetch(r).wait()
        for p in range(page):
            i = r * page + p
            for kt in range(lora // 128):
                y[i, kt * 128:(kt + 1) * 128] = y[i, kt * 128:(kt + 1) * 128].T
            xr = y[i, lora:k]
            y[i, lora:KP] = jnp.concatenate([xr, jnp.zeros((KP - k, b), xr.dtype)], 0).T
        return 0

    def seg(i, _):
        lax.fori_loop(i * (nr // g), (i + 1) * (nr // g), load, 0)

        @pl.when(i >= 1)
        def _():
            relay1(i - 1)

        @pl.when(i >= 3)
        def _():
            relay2(i - 3)
        return 0

    lax.fori_loop(0, g, seg, 0)
    relay1(g - 1)
    for i in range(g - 3, g):
        relay2(i)

    def rows(ti, tn, gi, nk):
        parts = [y[pl.ds(ti, tn), pl.ds(kt * 128 + gi * 16, 16)].reshape(tn * 16, 128) for kt in range(nk)]
        return jnp.concatenate(parts, axis=1)

    def loadq(gi):
        for kind in (2, 3, 5, 7):
            qwait(gi, kind)
        q0 = qall[gi, :, 0].reshape(128, KP)
        q1 = qall[gi, :, 1].reshape(128, KP)
        qt[...] = jnp.concatenate([q0, q1], axis=0).T

    def qk(gi, j, s_ref, m):
        s = jnp.dot(rows(j * TQ, TQ, gi, KP // 128), qt[...], preferred_element_type=jnp.float32)
        s = s.reshape(TQ, 2, 8, 256)
        ti = lax.broadcasted_iota(jnp.int32, (TQ, 1, 1), 0) + j * TQ
        pos = ((ti // page) * n + me) * page + lax.rem(ti, page)
        out = []
        for o in range(2):
            so = s[:, o, :, o * 128:(o + 1) * 128] * (SCALE * LOG2E)
            so = jnp.where(pos < lm_ref[gi, o][None], so, -jnp.inf)
            s_ref[o, pl.ds(j * TQ, TQ)] = so
            out.append(jnp.maximum(m[o], jnp.max(so, axis=0)))
        return tuple(out)

    def fin(m):
        return tuple(jnp.max(a, axis=0, keepdims=True) for a in m)

    def fix(m):
        return jnp.where(m == -jnp.inf, 0.0, m)

    lane = lax.broadcasted_iota(jnp.int32, (128, TV * 16), 1)
    first = lax.rem(lane, 16) < 8

    def pv(gi, j, s_ref, mf, l, acc):
        pe = []
        lo = []
        for o in range(2):
            p = jnp.exp2(s_ref[o, pl.ds(j * TV, TV)] - mf[o][None])
            lo.append(l[o] + jnp.sum(p, axis=0))
            pe.append(p)
        pm = jnp.concatenate(pe, axis=1).astype(jnp.bfloat16).reshape(TV * 16, 128).T
        z = jnp.zeros_like(pm)
        pt = jnp.concatenate([jnp.where(first, pm, z), jnp.where(first, z, pm)], axis=0)
        acc = acc + jnp.dot(pt, rows(j * TV, TV, gi, lora // 128), preferred_element_type=jnp.float32)
        return tuple(lo), acc

    def asend(gi):
        return rc(accs.at[gi, 1 - c], arecv.at[gi], ss.at[gi], sr.at[gi], at(0, False))

    def put(gi, m, l, acc):
        for o in range(2):
            lo = jnp.sum(l[o], axis=0, keepdims=True)
            st = jnp.concatenate([m[o], lo, jnp.zeros((6, 128), jnp.float32)], axis=0)
            for h in range(2):
                r0 = o * 128 + h * 64
                accs[gi, h, o, 0:64] = acc[r0:r0 + 64]
                accs[gi, h, o, 64:72, 0:128] = st
        asend(gi).start()

    def psend(gi, dx):
        return rc(part.at[gi, lax.rem(x + dx, nx)], precv.at[gi, 3 - dx], ps.at[gi, dx - 1], pr.at[gi, 3 - dx], at(dx, True))

    def lsend(gi, dx):
        return rc(lses.at[gi], lrecv.at[gi, 3 - dx], ls.at[gi, dx - 1], lr.at[gi, 3 - dx], at(dx, True))

    def merge(gi):
        asend(gi).wait_recv()
        for o in range(2):
            m1, l1 = accs[gi, c, o, 64:65, 0:128], accs[gi, c, o, 65:66, 0:128]
            m2, l2 = arecv[gi, o, 64:65, 0:128], arecv[gi, o, 65:66, 0:128]
            mm = jnp.maximum(m1, m2)
            ms = fix(mm)
            w1, w2 = jnp.exp2(m1 - ms), jnp.exp2(m2 - ms)
            lt = w1 * l1 + w2 * l2
            has = lt > 0.0
            lsafe = jnp.where(has, lt, 1.0)
            lses[gi, o:o + 1] = jnp.where(has, ms + jnp.log2(lsafe), -jnp.inf)
            wr = jnp.concatenate([w1 / lsafe, w2 / lsafe, jnp.zeros((6, 128), jnp.float32)], axis=0)
            cols[...] = wr.T
            w = cols[pl.ds(c * 64, 64)]
            od = accs[gi, c, o, 0:64] * w[:, 0:1] + arecv[gi, o, 0:64] * w[:, 1:2]
            part[gi, :, o] = od.astype(jnp.bfloat16).reshape(nx, 16, lora)
        for dx in (2, 1, 3):
            psend(gi, dx).start()
            lsend(gi, dx).start()

    def final(gi):
        for dx in range(1, 4):
            psend(gi, dx).wait_recv()
            lsend(gi, dx).wait_recv()
        for o in range(2):
            le = [lses[gi, o:o + 1]] + [lrecv[gi, i, o:o + 1] for i in range(3)]
            top = functools.reduce(jnp.maximum, le)
            w = [jnp.exp2(a - top) for a in le]
            tot = sum(w)
            wr = jnp.concatenate([a / tot for a in w] + [jnp.zeros((4, 128), jnp.float32)], axis=0)
            cols[...] = wr.T
            wc = cols[pl.ds(c * 64 + x * 16, 16)]
            od = part[gi, x, o].astype(jnp.float32) * wc[:, 0:1]
            for i in range(3):
                od = od + precv[gi, i, o].astype(jnp.float32) * wc[:, i + 1:i + 2]
            o_ref[gi, o] = od.astype(jnp.bfloat16)

    m0 = (jnp.full((8, 128), -jnp.inf, jnp.float32),) * 2
    l0 = (jnp.zeros((8, 128), jnp.float32),) * 2
    a0 = jnp.zeros((256, lora), jnp.float32)

    def after(ga):
        @pl.when(ga >= 1)
        def _():
            merge(ga - 1)

        @pl.when(ga >= 3)
        def _():
            final(ga - 3)

    def both(ga, sa, gb, sb, m):
        loadq(gb)
        mf = [fix(a) for a in m]
        mn, l, acc = m0, l0, a0
        for j in range(t // TQ):
            mn = qk(gb, j, sb, mn)
            l, acc = pv(ga, j, sa, mf, l, acc)
        put(ga, m, l, acc)
        after(ga)
        return fin(mn)

    def only_qk(gi, s_ref):
        loadq(gi)
        m = m0
        for j in range(t // TQ):
            m = qk(gi, j, s_ref, m)
        return fin(m)

    def only_pv(gi, s_ref, m):
        mf = [fix(a) for a in m]
        l, acc = l0, a0
        for j in range(t // TV):
            l, acc = pv(gi, j, s_ref, mf, l, acc)
        put(gi, m, l, acc)
        after(gi)

    def pair(i, m):
        m = both(2 * i, s0_ref, 2 * i + 1, s1_ref, m)
        return both(2 * i + 1, s1_ref, 2 * i + 2, s0_ref, m)

    m = only_qk(0, s0_ref)
    m = lax.fori_loop(0, g // 2 - 1, pair, m)
    m = both(g - 2, s0_ref, g - 1, s1_ref, m)
    only_pv(g - 1, s1_ref, m)
    merge(g - 1)
    for gi in range(g - 3, g):
        final(gi)

    def drain(gi, _):
        for kind in range(8):
            qsend(gi, kind).wait_send()
        asend(gi).wait_send()
        for dx in range(1, 4):
            psend(gi, dx).wait_send()
            lsend(gi, dx).wait_send()
        return 0

    lax.fori_loop(0, g, drain, 0)


def solution(mesh):
    n = mesh.shape['dcp']
    nx = n // 2

    def local(q, cache, lens):
        b, hl, k = q.shape
        nr, page = cache.shape[1], cache.shape[3]
        lora = k - ROPE
        g = b // 16
        t = nr * page
        qo = jnp.pad(q.reshape(g, 2, 16, k), [(0, 0)] * 3 + [(0, KP - k)])
        lane = jnp.arange(128)
        diag = (lane[None, :] // hl) % 8 == jnp.arange(8)[:, None]
        lm = jnp.where(diag, lens.reshape(g, 2, 8)[:, :, :, None], 0)
        ct = jnp.transpose(cache, (1, 2, 3, 4, 0)).reshape(nr, page, k, b)
        o = pl.pallas_call(
            kernel,
            out_shape=jax.ShapeDtypeStruct((g, 2, 16, lora), jnp.bfloat16),
            in_specs=[pl.BlockSpec(memory_space=pltpu.VMEM)] * 2 + [pl.BlockSpec(memory_space=pl.ANY)],
            out_specs=pl.BlockSpec(memory_space=pltpu.VMEM),
            scratch_shapes=[
                pltpu.VMEM((t, KP, b), jnp.bfloat16),
                pltpu.VMEM((g, n, 2, 16, KP), jnp.bfloat16),
                pltpu.VMEM((KP, 256), jnp.bfloat16),
                pltpu.VMEM((2, t, 8, 128), jnp.float32),
                pltpu.VMEM((2, t, 8, 128), jnp.float32),
                pltpu.VMEM((g, 2, 2, 72, lora), jnp.float32),
                pltpu.VMEM((g, 2, 72, lora), jnp.float32),
                pltpu.VMEM((g, nx, 2, 16, lora), jnp.bfloat16),
                pltpu.VMEM((g, nx - 1, 2, 16, lora), jnp.bfloat16),
                pltpu.VMEM((g, 2, 128), jnp.float32),
                pltpu.VMEM((g, nx - 1, 2, 128), jnp.float32),
                pltpu.VMEM((128, 8), jnp.float32),
                pltpu.SemaphoreType.DMA((nr,)),
                pltpu.SemaphoreType.DMA((g, 8)),
                pltpu.SemaphoreType.DMA((g, 8)),
                pltpu.SemaphoreType.DMA((g,)),
                pltpu.SemaphoreType.DMA((g,)),
                pltpu.SemaphoreType.DMA((g, nx - 1)),
                pltpu.SemaphoreType.DMA((g, nx - 1)),
                pltpu.SemaphoreType.DMA((g, nx - 1)),
                pltpu.SemaphoreType.DMA((g, nx - 1)),
            ],
            compiler_params=pltpu.CompilerParams(vmem_limit_bytes=67043328, collective_id=0, has_side_effects=True),
        )(lm, qo, ct)
        return o.reshape(b, hl, lora)

    return jax.shard_map(local, mesh=mesh, in_specs=(P('dp', 'dcp', None), P('dp', None, 'dcp', None, None), P('dp')), out_specs=P('dp', 'dcp', None), check_vma=False)
```

```python
import functools
import jax
import jax.numpy as jnp
from jax import lax
from jax.experimental import pallas as pl
from jax.experimental.pallas import tpu as pltpu
from jax.sharding import PartitionSpec as P

ROPE = 64
QK_DIM = 192
SCALE = QK_DIM ** -0.5
LOG2E = 1.4426950408889634
KP = 640
TQ = 64
TV = 64
MESH = pl.DeviceIdType.MESH


def kernel(lens_ref, qn_ref, c_hbm, o_ref, y, q_ref, lm_ref, qall, qt, s0_ref, s1_ref, accs, arecv, part, precv, lses, lrecv, cols,
           csem, qs, qr, ss, sr, ps, pr, ls, lr):
    me = lax.axis_index('dcp')
    dp = lax.axis_index('dp')
    x, c = me // 2, lax.rem(me, 2)
    nx = 4
    n = 2 * nx
    nr, page, k, b = c_hbm.shape
    g = b // 16
    t = nr * page
    lora = k - ROPE
    bf = jnp.bfloat16
    f32 = jnp.float32

    def at(dx, same):
        xx = lax.rem(x + dx + nx, nx)
        return (dp, xx * 2 + (c if same else 1 - c))

    def slot(dx):
        return c * nx + lax.rem(x + dx + nx, nx)

    def pslot(dx):
        return (1 - c) * nx + lax.rem(x + dx + nx, nx)

    def fetch(r):
        return pltpu.make_async_copy(c_hbm.at[r], y.at[pl.ds(r * page, page), 0:k], csem.at[r])

    for r in range(nr):
        fetch(r).start()

    barrier = pltpu.get_barrier_semaphore()
    for dev in (at(1, True), at(-1, True), at(2, True), at(0, False)):
        pl.semaphore_signal(barrier, inc=1, device_id=dev, device_id_type=MESH)

    for kt in range(KP // 128):
        r0, r1 = kt * 128, min(kt * 128 + 128, k)
        hs = []
        for h in range(2):
            xq = qn_ref[h, r0:r1]
            if r1 - r0 < 128:
                xq = jnp.concatenate([xq, jnp.zeros((128 - (r1 - r0), b), bf)], 0)
            hs.append(xq.T.astype(f32).reshape(g, 2, 1, 8, 128))
        q_ref[:, :, :, r0:r0 + 128] = jnp.concatenate(hs, axis=2).reshape(g, 2, 16, 128).astype(bf)

    sub = lax.broadcasted_iota(jnp.int32, (8, 128), 0)
    diag = lax.rem(lax.broadcasted_iota(jnp.int32, (8, 128), 1), 8) == sub
    for gi in range(g):
        for o in range(2):
            v = jnp.zeros((8, 128), jnp.int32)
            for i in range(8):
                v = jnp.where(sub == i, lens_ref[gi * 16 + o * 8 + i], v)
            lm_ref[gi, o] = jnp.where(diag, v, 0)

    pl.semaphore_wait(barrier, 4)

    def rc(src, dst, s, r, dev):
        return pltpu.make_async_remote_copy(src_ref=src, dst_ref=dst, send_sem=s, recv_sem=r, device_id=dev, device_id_type=MESH)

    def qsend(gi, kind):
        sl = {0: slot(0), 1: slot(0), 2: slot(0), 3: slot(-1), 4: slot(-1), 5: slot(1), 6: slot(1), 7: slot(2)}[kind]
        dev = {0: at(1, True), 1: at(-1, True), 4: at(1, True), 6: at(-1, True)}.get(kind, at(0, False))
        half = {4: 0, 6: 1}.get(kind)
        if kind <= 2:
            src, dst = q_ref.at[gi], qall.at[gi, sl]
        elif half is None:
            src = dst = qall.at[gi, sl]
        else:
            src = dst = qall.at[gi, sl, half]
        return rc(src, dst, qs.at[gi, kind], qr.at[gi, kind], dev)

    def qwait(gi, kind):
        sl = {0: slot(-1), 1: slot(1), 2: pslot(0), 3: pslot(-1), 4: slot(2), 5: pslot(1), 6: slot(2), 7: pslot(2)}[kind]
        half = {4: 0, 6: 1}.get(kind)
        ref = qall.at[gi, sl] if half is None else qall.at[gi, sl, half]
        rc(ref, ref, qs.at[gi, kind], qr.at[gi, kind], at(0, False)).wait_recv()

    for gi in range(g):
        for kind in range(3):
            qsend(gi, kind).start()
        qall[gi, slot(0)] = q_ref[gi]

    def relay1(gi):
        qwait(gi, 0)
        qsend(gi, 4).start()
        qsend(gi, 3).start()
        qwait(gi, 1)
        qsend(gi, 6).start()
        qsend(gi, 5).start()

    def relay2(gi):
        qwait(gi, 4)
        qwait(gi, 6)
        qsend(gi, 7).start()

    def load(r, _):
        fetch(r).wait()
        for p in range(page):
            i = r * page + p
            for kt in range(lora // 128):
                y[i, kt * 128:(kt + 1) * 128] = y[i, kt * 128:(kt + 1) * 128].T
            xr = y[i, lora:k]
            y[i, lora:KP] = jnp.concatenate([xr, jnp.zeros((KP - k, b), xr.dtype)], 0).T
        return 0

    def step(r, _):
        load(r, 0)
        u = r - 6
        for j, f in ((u, relay1), (u - 7, relay2)):
            @pl.when((j >= 0) & (lax.rem(j + 30, 3) == 0) & (j < 3 * g))
            def _():
                f(j // 3)
        return 0

    lax.fori_loop(0, nr, step, 0)

    def rows(ti, tn, gi, nk):
        parts = [y[pl.ds(ti, tn), pl.ds(kt * 128 + gi * 16, 16)].reshape(tn * 16, 128) for kt in range(nk)]
        return jnp.concatenate(parts, axis=1)

    def loadq(gi):
        for kind in (2, 3, 5, 7):
            qwait(gi, kind)
        q0 = qall[gi, :, 0].reshape(128, KP)
        q1 = qall[gi, :, 1].reshape(128, KP)
        qt[...] = jnp.concatenate([q0, q1], axis=0).T

    def qk(gi, j, s_ref, m):
        s = jnp.dot(rows(j * TQ, TQ, gi, KP // 128), qt[...], preferred_element_type=jnp.float32)
        s = s.reshape(TQ, 2, 8, 256)
        ti = lax.broadcasted_iota(jnp.int32, (TQ, 1, 1), 0) + j * TQ
        pos = ((ti // page) * n + me) * page + lax.rem(ti, page)
        out = []
        for o in range(2):
            so = s[:, o, :, o * 128:(o + 1) * 128] * (SCALE * LOG2E)
            so = jnp.where(pos < lm_ref[gi, o][None], so, -jnp.inf)
            s_ref[o, pl.ds(j * TQ, TQ)] = so
            out.append(jnp.maximum(m[o], jnp.max(so, axis=0)))
        return tuple(out)

    def fin(m):
        return tuple(jnp.max(a, axis=0, keepdims=True) for a in m)

    def fix(m):
        return jnp.where(m == -jnp.inf, 0.0, m)

    lane = lax.broadcasted_iota(jnp.int32, (128, TV * 16), 1)
    first = lax.rem(lane, 16) < 8

    def pv(gi, j, s_ref, mf, l, acc):
        pe = []
        lo = []
        for o in range(2):
            p = jnp.exp2(s_ref[o, pl.ds(j * TV, TV)] - mf[o][None])
            lo.append(l[o] + jnp.sum(p, axis=0))
            pe.append(p)
        pm = jnp.concatenate(pe, axis=1).astype(jnp.bfloat16).reshape(TV * 16, 128).T
        z = jnp.zeros_like(pm)
        pt = jnp.concatenate([jnp.where(first, pm, z), jnp.where(first, z, pm)], axis=0)
        acc = acc + jnp.dot(pt, rows(j * TV, TV, gi, lora // 128), preferred_element_type=jnp.float32)
        return tuple(lo), acc

    def asend(gi):
        return rc(accs.at[gi, 1 - c], arecv.at[gi], ss.at[gi], sr.at[gi], at(0, False))

    def put(gi, m, l, acc):
        for o in range(2):
            lo = jnp.sum(l[o], axis=0, keepdims=True)
            st = jnp.concatenate([m[o], lo, jnp.zeros((6, 128), jnp.float32)], axis=0)
            for h in range(2):
                r0 = o * 128 + h * 64
                accs[gi, h, o, 0:64] = acc[r0:r0 + 64]
                accs[gi, h, o, 64:72, 0:128] = st
        asend(gi).start()

    def psend(gi, dx):
        return rc(part.at[gi, lax.rem(x + dx, nx)], precv.at[gi, 3 - dx], ps.at[gi, dx - 1], pr.at[gi, 3 - dx], at(dx, True))

    def lsend(gi, dx):
        return rc(lses.at[gi], lrecv.at[gi, 3 - dx], ls.at[gi, dx - 1], lr.at[gi, 3 - dx], at(dx, True))

    def merge_wait(gi):
        asend(gi).wait_recv()

    def merge(gi):
        for o in range(2):
            m1, l1 = accs[gi, c, o, 64:65, 0:128], accs[gi, c, o, 65:66, 0:128]
            m2, l2 = arecv[gi, o, 64:65, 0:128], arecv[gi, o, 65:66, 0:128]
            mm = jnp.maximum(m1, m2)
            ms = fix(mm)
            w1, w2 = jnp.exp2(m1 - ms), jnp.exp2(m2 - ms)
            lt = w1 * l1 + w2 * l2
            has = lt > 0.0
            lsafe = jnp.where(has, lt, 1.0)
            lses[gi, o:o + 1] = jnp.where(has, ms + jnp.log2(lsafe), -jnp.inf)
            wr = jnp.concatenate([w1 / lsafe, w2 / lsafe, jnp.zeros((6, 128), f32)], axis=0)
            cols[o] = wr.T
            w = cols[o, pl.ds(c * 64, 64)]
            od = accs[gi, c, o, 0:64] * w[:, 0:1] + arecv[gi, o, 0:64] * w[:, 1:2]
            part[gi, :, o] = od.astype(bf).reshape(nx, 16, lora)

    def merge_send(gi):
        for dx in (2, 1, 3):
            psend(gi, dx).start()
            lsend(gi, dx).start()

    def final_wait(gi):
        for dx in range(1, 4):
            psend(gi, dx).wait_recv()
            lsend(gi, dx).wait_recv()

    def final(gi):
        for o in range(2):
            le = [lses[gi, o:o + 1]] + [lrecv[gi, i, o:o + 1] for i in range(3)]
            top = functools.reduce(jnp.maximum, le)
            w = [jnp.exp2(a - top) for a in le]
            tot = sum(w)
            wr = jnp.concatenate([a / tot for a in w] + [jnp.zeros((4, 128), f32)], axis=0)
            cols[2 + o] = wr.T
            wc = cols[2 + o, pl.ds(c * 64 + x * 16, 16)]
            od = part[gi, x, o].astype(f32) * wc[:, 0:1]
            for i in range(3):
                od = od + precv[gi, i, o].astype(f32) * wc[:, i + 1:i + 2]
            o_ref[gi, o] = od.astype(bf)

    m0 = (jnp.full((8, 128), -jnp.inf, jnp.float32),) * 2
    l0 = (jnp.zeros((8, 128), jnp.float32),) * 2
    a0 = jnp.zeros((256, lora), jnp.float32)

    LAG = 4

    def top(ga):
        @pl.when(ga >= 1)
        def _():
            merge_wait(ga - 1)

        @pl.when(ga >= LAG)
        def _():
            final_wait(ga - LAG)

    def mid(ga):
        merge(lax.select(ga >= 1, ga - 1, g))
        final(lax.select(ga >= LAG, ga - LAG, g))

    def end(ga, m, l, acc):
        @pl.when(ga >= 1)
        def _():
            merge_send(ga - 1)
        put(ga, m, l, acc)

    def both(ga, sa, gb, sb, m):
        top(ga)
        loadq(gb)
        mid(ga)
        mf = [fix(a) for a in m]
        mn, l, acc = m0, l0, a0
        for j in range(t // TQ):
            mn = qk(gb, j, sb, mn)
            l, acc = pv(ga, j, sa, mf, l, acc)
        end(ga, m, l, acc)
        return fin(mn)

    def only_qk(gi, s_ref):
        loadq(gi)
        m = m0
        for j in range(t // TQ):
            m = qk(gi, j, s_ref, m)
        return fin(m)

    def only_pv(gi, s_ref, m):
        top(gi)
        mid(gi)
        mf = [fix(a) for a in m]
        l, acc = l0, a0
        for j in range(t // TV):
            l, acc = pv(gi, j, s_ref, mf, l, acc)
        end(gi, m, l, acc)

    def pair(i, m):
        m = both(2 * i, s0_ref, 2 * i + 1, s1_ref, m)
        return both(2 * i + 1, s1_ref, 2 * i + 2, s0_ref, m)

    m = only_qk(0, s0_ref)
    for i in range((nr - 13 + 2) // 3, g):
        relay2(i)
    m = lax.fori_loop(0, g // 2 - 1, pair, m)
    last = jnp.int32(g - 1)
    m = both(last - 1, s0_ref, last, s1_ref, m)
    only_pv(last, s1_ref, m)
    for gi in range(g - LAG, g - 2):
        final_wait(gi)
        final(gi)
    merge_wait(g - 1)
    merge(g - 1)
    merge_send(g - 1)
    for gi in range(g - 2, g):
        final_wait(gi)
        final(gi)

    def drain(gi, _):
        for kind in range(8):
            qsend(gi, kind).wait_send()
        asend(gi).wait_send()
        for dx in range(1, 4):
            psend(gi, dx).wait_send()
            lsend(gi, dx).wait_send()
        return 0

    lax.fori_loop(0, g, drain, 0)


def solution(mesh):
    n = mesh.shape['dcp']
    nx = n // 2

    def local(q, cache, lens):
        b, hl, k = q.shape
        nr, page = cache.shape[1], cache.shape[3]
        lora = k - ROPE
        g = b // 16
        t = nr * page
        qn = jnp.transpose(q, (1, 2, 0))
        ct = jnp.transpose(cache, (1, 2, 3, 4, 0)).reshape(nr, page, k, b)
        o = pl.pallas_call(
            kernel,
            out_shape=jax.ShapeDtypeStruct((g + 1, 2, 16, lora), jnp.bfloat16),
            in_specs=[pl.BlockSpec(memory_space=pltpu.SMEM), pl.BlockSpec(memory_space=pltpu.VMEM), pl.BlockSpec(memory_space=pl.ANY)],
            out_specs=pl.BlockSpec(memory_space=pltpu.VMEM),
            scratch_shapes=[
                pltpu.VMEM((t, KP, b), jnp.bfloat16),
                pltpu.VMEM((g, 2, 16, KP), jnp.bfloat16),
                pltpu.VMEM((g, 2, 8, 128), jnp.int32),
                pltpu.VMEM((g, n, 2, 16, KP), jnp.bfloat16),
                pltpu.VMEM((KP, 256), jnp.bfloat16),
                pltpu.VMEM((2, t, 8, 128), jnp.float32),
                pltpu.VMEM((2, t, 8, 128), jnp.float32),
                pltpu.VMEM((g + 1, 2, 2, 72, lora), jnp.float32),
                pltpu.VMEM((g + 1, 2, 72, lora), jnp.float32),
                pltpu.VMEM((g + 1, nx, 2, 16, lora), jnp.bfloat16),
                pltpu.VMEM((g + 1, nx - 1, 2, 16, lora), jnp.bfloat16),
                pltpu.VMEM((g + 1, 2, 128), jnp.float32),
                pltpu.VMEM((g + 1, nx - 1, 2, 128), jnp.float32),
                pltpu.VMEM((4, 128, 8), jnp.float32),
                pltpu.SemaphoreType.DMA((nr,)),
                pltpu.SemaphoreType.DMA((g, 8)),
                pltpu.SemaphoreType.DMA((g, 8)),
                pltpu.SemaphoreType.DMA((g,)),
                pltpu.SemaphoreType.DMA((g,)),
                pltpu.SemaphoreType.DMA((g, nx - 1)),
                pltpu.SemaphoreType.DMA((g, nx - 1)),
                pltpu.SemaphoreType.DMA((g, nx - 1)),
                pltpu.SemaphoreType.DMA((g, nx - 1)),
            ],
            compiler_params=pltpu.CompilerParams(vmem_limit_bytes=67043328, collective_id=0, has_side_effects=True),
        )(lens, qn, ct)
        return o[:g].reshape(g, 2, hl, 8, lora).transpose(0, 1, 3, 2, 4).reshape(b, hl, lora)

    return jax.shard_map(local, mesh=mesh, in_specs=(P('dp', 'dcp', None), P('dp', None, 'dcp', None, None), P('dp')), out_specs=P('dp', 'dcp', None), check_vma=False)
```

```python
import functools
import jax
import jax.numpy as jnp
from jax import lax
from jax.experimental import pallas as pl
from jax.experimental.pallas import tpu as pltpu
from jax.sharding import PartitionSpec as P

ROPE = 64
QK_DIM = 192
SCALE = QK_DIM ** -0.5
LOG2E = 1.4426950408889634
KP = 640
TQ = 64
TV = 64
NS = 4
NU = 4
MESH = pl.DeviceIdType.MESH


def kernel(lens_ref, qn_ref, c_hbm, o_ref, ylo, yhi, q_ref, lm_ref, qall, qt, s0_ref, s1_ref, accs, arecv, part, precv, lses, lrecv, cols,
           csem, qs, qr, ss, sr, ps, pr, ls, lr):
    me = lax.axis_index('dcp')
    dp = lax.axis_index('dp')
    x, c = me // 2, lax.rem(me, 2)
    nx = 4
    n = 2 * nx
    nr, page, k, b = c_hbm.shape
    g = b // 16
    t = nr * page
    lora = k - ROPE
    bf = jnp.bfloat16
    f32 = jnp.float32

    def at(dx, same):
        xx = lax.rem(x + dx + nx, nx)
        return (dp, xx * 2 + (c if same else 1 - c))

    def slot(dx):
        return c * nx + lax.rem(x + dx + nx, nx)

    def pslot(dx):
        return (1 - c) * nx + lax.rem(x + dx + nx, nx)

    def fetch(r, y):
        return pltpu.make_async_copy(c_hbm.at[r], y.at[pl.ds(lax.rem(r, nr // 2) * page, page), 0:k], csem.at[r])

    for r in range(nr):
        fetch(r, ylo if r < nr // 2 else yhi).start()

    barrier = pltpu.get_barrier_semaphore()
    for dev in (at(1, True), at(-1, True), at(2, True), at(0, False)):
        pl.semaphore_signal(barrier, inc=1, device_id=dev, device_id_type=MESH)

    for kt in range(KP // 128):
        r0, r1 = kt * 128, min(kt * 128 + 128, k)
        hs = []
        for h in range(2):
            xq = qn_ref[h, r0:r1]
            if r1 - r0 < 128:
                xq = jnp.concatenate([xq, jnp.zeros((128 - (r1 - r0), b), bf)], 0)
            hs.append(xq.T.astype(f32).reshape(g, 2, 1, 8, 128))
        q_ref[:, :, :, r0:r0 + 128] = jnp.concatenate(hs, axis=2).reshape(g, 2, 16, 128).astype(bf)

    sub = lax.broadcasted_iota(jnp.int32, (8, 128), 0)
    lane8 = lax.rem(lax.broadcasted_iota(jnp.int32, (8, 128), 1), 8)
    diag = lane8 == sub
    turn = lax.rem(sub - lane8 + 8, 8)
    for gi in range(g):
        for o in range(2):
            v = jnp.zeros((8, 128), jnp.int32)
            for i in range(8):
                v = jnp.where(lane8 == i, lens_ref[gi * 16 + o * 8 + i], v)
            lm_ref[gi, o] = v

    def load(r, y):
        for i in range(2):
            fetch(2 * r + i, y).wait()
        for p in range(2 * page):
            i = lax.rem(r, nr // 4) * 2 * page + p
            for kt in range(lora // 128):
                y[i, kt * 128:(kt + 1) * 128] = y[i, kt * 128:(kt + 1) * 128].T
            xr = y[i, lora:k]
            y[i, lora:KP] = jnp.concatenate([xr, jnp.zeros((KP - k, b), xr.dtype)], 0).T

    load(0, ylo)
    pl.semaphore_wait(barrier, 4)

    def rc(src, dst, s, r, dev):
        return pltpu.make_async_remote_copy(src_ref=src, dst_ref=dst, send_sem=s, recv_sem=r, device_id=dev, device_id_type=MESH)

    def qsend(gi, kind):
        sl = {0: slot(0), 1: slot(0), 2: slot(0), 3: slot(-1), 4: slot(-1), 5: slot(1), 6: slot(1), 7: slot(2)}[kind]
        dev = {0: at(1, True), 1: at(-1, True), 4: at(1, True), 6: at(-1, True)}.get(kind, at(0, False))
        half = {4: 0, 6: 1}.get(kind)
        if kind <= 2:
            src, dst = q_ref.at[gi], qall.at[gi, sl]
        elif half is None:
            src = dst = qall.at[gi, sl]
        else:
            src = dst = qall.at[gi, sl, half]
        return rc(src, dst, qs.at[gi, kind], qr.at[gi, kind], dev)

    def qwait(gi, kind):
        sl = {0: slot(-1), 1: slot(1), 2: pslot(0), 3: pslot(-1), 4: slot(2), 5: pslot(1), 6: slot(2), 7: pslot(2)}[kind]
        half = {4: 0, 6: 1}.get(kind)
        ref = qall.at[gi, sl] if half is None else qall.at[gi, sl, half]
        rc(ref, ref, qs.at[gi, kind], qr.at[gi, kind], at(0, False)).wait_recv()

    AHEAD = 3

    def own(gi):
        for kind in range(3):
            qsend(gi, kind).start()

    for gi in range(AHEAD):
        own(gi)
    for gi in range(g):
        qall[gi, slot(0)] = q_ref[gi]

    def relay1(gi):
        qwait(gi, 0)
        qsend(gi, 4).start()
        qsend(gi, 3).start()
        qwait(gi, 1)
        qsend(gi, 6).start()
        qsend(gi, 5).start()

        @pl.when(gi + AHEAD < g)
        def _():
            own(gi + AHEAD)

    def relay2(gi):
        qwait(gi, 4)
        qwait(gi, 6)
        qsend(gi, 7).start()

    R1, R2 = 4, 8

    def relays(r):
        for rr, f in ((R1, relay1), (R2, relay2)):
            j = r - rr

            @pl.when((j >= 0) & (lax.rem(j + 30, 3) == 0) & (2 * (j // 3) < g))
            def _():
                f(2 * (j // 3))

            @pl.when((j >= 2) & (lax.rem(j + 28, 3) == 0) & (2 * ((j - 2) // 3) + 1 < g))
            def _():
                f(2 * ((j - 2) // 3) + 1)

    def count(rr):
        return len([gi for gi in range(g) if rr + (3 * gi + 1) // 2 < nr // 2])

    n1, n2 = count(R1), count(R2)

    def rows(ti, tn, gi, nk):
        y = ylo if ti < t // 2 else yhi
        ti = ti % (t // 2)
        parts = [y[pl.ds(ti, tn), pl.ds(kt * 128 + gi * 16, 16)].reshape(tn * 16, 128) for kt in range(nk)]
        return jnp.concatenate(parts, axis=1)

    def loadq(gi):
        for kind in (2, 3, 5, 7):
            qwait(gi, kind)
        reload(gi)

    def reload(gi):
        q0 = qall[gi, :, 0].reshape(128, KP)
        q1 = qall[gi, :, 1].reshape(128, KP)
        qt[...] = jnp.concatenate([q0, q1], axis=0).T

    def qk(gi, j, s_ref):
        s = jnp.dot(rows(j * TQ, TQ, gi, KP // 128), qt[...], preferred_element_type=jnp.float32)
        s = s.reshape(TQ // 8, 8, 2, 8, 256)
        blk = lax.broadcasted_iota(jnp.int32, (TQ // 8, 1, 1), 0) + j * (TQ // 8)
        pos = (blk * n + me) * page + turn[None]
        for o in range(2):
            d = s[:, 0, o, :, o * 128:(o + 1) * 128]
            for i in range(1, 8):
                d = jnp.where((turn == i)[None], pltpu.roll(s[:, i, o, :, o * 128:(o + 1) * 128], i, 1), d)
            d = jnp.where(pos < lm_ref[gi, o][None], d * (SCALE * LOG2E), -jnp.inf)
            s_ref[gi // 2, o, pl.ds(j * (TQ // 8), TQ // 8)] = d

    def qks(gi, j0, j1, s_ref):
        for j in range(j0, j1):
            qk(gi, j, s_ref)

    def fix(m):
        return jnp.where(m == -jnp.inf, 0.0, m)

    def maxes(gi, s_ref):
        return [jnp.max(jnp.max(s_ref[gi // 2, o], axis=0), axis=0, keepdims=True) for o in range(2)]

    lane = lax.broadcasted_iota(jnp.int32, (128, TV * 16), 1)
    first = lax.rem(lane, 16) < 8

    def pv(gi, j, s_ref, mf, l, acc):
        pe = []
        lo = []
        for o in range(2):
            p = jnp.exp2(s_ref[gi // 2, o, pl.ds(j * (TV // 8), TV // 8)] - mf[o][None])
            lo.append(l[o] + jnp.sum(p, axis=0))
            q = [p] + [pltpu.roll(p, 8 - i, 1) for i in range(1, 8)]
            q = jnp.stack([jnp.where(diag[None], a, 0.0) for a in q], axis=1)
            pe.append(q.reshape(TV, 8, 128))
        pm = jnp.concatenate(pe, axis=1).astype(bf).reshape(TV * 16, 128).T
        z = jnp.zeros_like(pm)
        pt = jnp.concatenate([jnp.where(first, pm, z), jnp.where(first, z, pm)], axis=0)
        acc = acc + jnp.dot(pt, rows(j * TV, TV, gi, lora // 128), preferred_element_type=jnp.float32)
        return tuple(lo), acc

    def asend(gi):
        return rc(accs.at[lax.rem(gi, NS), 1 - c], arecv.at[lax.rem(gi, NS)], ss.at[gi], sr.at[gi], at(0, False))

    def put(gi, m, l, acc):
        gs = lax.rem(gi, NS)

        @pl.when(gi >= NS)
        def _():
            asend(gi - NS).wait_send()

        for o in range(2):
            lo = jnp.sum(l[o], axis=0, keepdims=True)
            st = jnp.concatenate([m[o], lo, jnp.zeros((6, 128), jnp.float32)], axis=0)
            for h in range(2):
                r0 = o * 128 + h * 64
                accs[gs, h, o, 0:64] = acc[r0:r0 + 64]
                accs[gs, h, o, 64:72, 0:128] = st
        asend(gi).start()

    def psend(gi, dx):
        return rc(part.at[gi, lax.rem(x + dx, nx)], precv.at[gi, 3 - dx], ps.at[gi, dx - 1], pr.at[gi, 3 - dx], at(dx, True))

    def lsend(gi, dx):
        return rc(lses.at[gi], lrecv.at[gi, 3 - dx], ls.at[gi, dx - 1], lr.at[gi, 3 - dx], at(dx, True))

    def merge_wait(gi):
        asend(gi).wait_recv()

    def merge(gi, live=None):
        gs = lax.rem(gi, NS)
        if live is not None:
            gs, gi = lax.select(live, gs, NS), lax.select(live, gi, g)
        for o in range(2):
            m1, l1 = accs[gs, c, o, 64:65, 0:128], accs[gs, c, o, 65:66, 0:128]
            m2, l2 = arecv[gs, o, 64:65, 0:128], arecv[gs, o, 65:66, 0:128]
            mm = jnp.maximum(m1, m2)
            ms = fix(mm)
            w1, w2 = jnp.exp2(m1 - ms), jnp.exp2(m2 - ms)
            lt = w1 * l1 + w2 * l2
            has = lt > 0.0
            lsafe = jnp.where(has, lt, 1.0)
            lses[gi, o:o + 1] = jnp.where(has, ms + jnp.log2(lsafe), -jnp.inf)
            wr = jnp.concatenate([w1 / lsafe, w2 / lsafe, jnp.zeros((6, 128), f32)], axis=0)
            cols[o] = wr.T
            w = cols[o, pl.ds(c * 64, 64)]
            od = accs[gs, c, o, 0:64] * w[:, 0:1] + arecv[gs, o, 0:64] * w[:, 1:2]
            part[gi, :, o] = od.astype(bf).reshape(nx, 16, lora)

    def merge_send(gi):
        for dx in (2, 1, 3):
            psend(gi, dx).start()
            lsend(gi, dx).start()

    def final_wait(gi):
        for dx in range(1, 4):
            psend(gi, dx).wait_recv()
            lsend(gi, dx).wait_recv()

    def final(gi, live=None):
        og = gi
        if live is not None:
            og, gi = lax.select(live, gi, 0), lax.select(live, gi, g)
        for o in range(2):
            le = [lses[gi, o:o + 1]] + [lrecv[gi, i, o:o + 1] for i in range(3)]
            top = functools.reduce(jnp.maximum, le)
            w = [jnp.exp2(a - top) for a in le]
            tot = sum(w)
            wr = jnp.concatenate([a / tot for a in w] + [jnp.zeros((4, 128), f32)], axis=0)
            cols[2 + o] = wr.T
            wc = cols[2 + o, pl.ds(c * 64 + x * 16, 16)]
            od = part[gi, x, o].astype(f32) * wc[:, 0:1]
            for i in range(3):
                od = od + precv[gi, i, o].astype(f32) * wc[:, i + 1:i + 2]
            o_ref[pl.ds(og * 16 + o * 8, 8)] = jnp.stack([od[0:8], od[8:16]], axis=1).astype(bf)

    l0 = (jnp.zeros((8, 128), jnp.float32),) * 2
    a0 = jnp.zeros((256, lora), jnp.float32)

    LAG = 5
    ML = 2

    def top(ga):
        @pl.when(ga + n1 < g)
        def _():
            relay1(ga + n1)

        @pl.when(ga + n2 < g)
        def _():
            relay2(ga + n2)

        @pl.when(ga >= ML)
        def _():
            merge_wait(ga - ML)

        @pl.when(ga >= LAG)
        def _():
            final_wait(ga - LAG)

    def mid(ga):
        merge(lax.rem(ga - ML + NS * g, NS * g), ga >= ML)
        final(ga - LAG, ga >= LAG)

    def end(ga, m, l, acc):
        @pl.when(ga >= ML)
        def _():
            merge_send(ga - ML)
        put(ga, m, l, acc)

    NJ = t // TQ

    def both(ga, sa, gb, sb, j0):
        top(ga)
        (reload if j0 else loadq)(gb)
        mid(ga)
        m = maxes(ga, sa)
        mf = [fix(a) for a in m]
        l, acc = l0, a0
        done = j0
        for j in range(NJ):
            todo = j0 + (NJ - j0) * (j + 1) // NJ
            qks(gb, done, todo, sb)
            done = todo
            l, acc = pv(ga, j, sa, mf, l, acc)
        end(ga, m, l, acc)

    def only_pv(gi, s_ref):
        top(gi)
        mid(gi)
        m = maxes(gi, s_ref)
        mf = [fix(a) for a in m]
        l, acc = l0, a0
        for j in range(NJ):
            l, acc = pv(gi, j, s_ref, mf, l, acc)
        end(gi, m, l, acc)

    def pair(i, _, j0):
        both(2 * i, s0_ref, 2 * i + 1, s1_ref, j0)
        both(2 * i + 1, s1_ref, 2 * i + 2, s0_ref, j0)
        return 0

    H = NJ // 2
    U0 = nr // 2 - NU

    def astep(r, _, y):
        relays(r)
        load(r, y)
        return 0

    def bstep(i, _):
        for s_ref, e in ((s0_ref, 0), (s1_ref, 1)):
            r = U0 + 2 * i + e
            relays(r)
            loadq(2 * i + e)
            load(r, yhi)
            qks(2 * i + e, 0, H, s_ref)
        return 0

    lax.fori_loop(1, nr // 4, functools.partial(astep, y=ylo), 0)
    lax.fori_loop(nr // 4, U0, functools.partial(astep, y=yhi), 0)
    lax.fori_loop(0, NU // 2, bstep, 0)
    reload(0)
    qks(0, H, NJ, s0_ref)
    lax.fori_loop(0, NU // 2 - 1, functools.partial(pair, j0=H), 0)
    both(jnp.int32(NU - 2), s0_ref, jnp.int32(NU - 1), s1_ref, H)
    both(jnp.int32(NU - 1), s1_ref, jnp.int32(NU), s0_ref, 0)
    lax.fori_loop(NU // 2, g // 2 - 1, functools.partial(pair, j0=0), 0)
    last = jnp.int32(g - 1)
    both(last - 1, s0_ref, last, s1_ref, 0)
    only_pv(last, s1_ref)
    for gi in range(g - ML, g - 1):
        merge_wait(gi)
        merge(gi)
        merge_send(gi)
    for gi in range(g - LAG, g - ML - 1):
        final_wait(gi)
        final(gi)
    merge_wait(g - 1)
    merge(g - 1)
    merge_send(g - 1)
    def drain(gi, _):
        for kind in range(8):
            qsend(gi, kind).wait_send()
        @pl.when(gi >= g - NS)
        def _():
            asend(gi).wait_send()

        for dx in range(1, 4):
            psend(gi, dx).wait_send()
            lsend(gi, dx).wait_send()
        return 0

    lax.fori_loop(0, g, drain, 0)

    for gi in range(g - ML - 1, g):
        final_wait(gi)
        final(gi)


def solution(mesh):
    n = mesh.shape['dcp']
    nx = n // 2

    def local(q, cache, lens):
        b, hl, k = q.shape
        nr, page = cache.shape[1], cache.shape[3]
        lora = k - ROPE
        g = b // 16
        t = nr * page
        qn = jnp.transpose(q, (1, 2, 0))
        ct = jnp.transpose(cache, (1, 2, 3, 4, 0)).reshape(nr, page, k, b)
        o = pl.pallas_call(
            kernel,
            out_shape=jax.ShapeDtypeStruct((b, hl, lora), jnp.bfloat16),
            in_specs=[pl.BlockSpec(memory_space=pltpu.SMEM), pl.BlockSpec(memory_space=pltpu.VMEM), pl.BlockSpec(memory_space=pl.ANY)],
            out_specs=pl.BlockSpec(memory_space=pltpu.VMEM),
            scratch_shapes=[
                pltpu.VMEM((t // 2, KP, b), jnp.bfloat16),
                pltpu.VMEM((t // 2, KP, b), jnp.bfloat16),
                pltpu.VMEM((g, 2, 16, KP), jnp.bfloat16),
                pltpu.VMEM((g, 2, 8, 128), jnp.int32),
                pltpu.VMEM((g, n, 2, 16, KP), jnp.bfloat16),
                pltpu.VMEM((KP, 256), jnp.bfloat16),
                pltpu.VMEM((g // 2, 2, t // 8, 8, 128), jnp.float32),
                pltpu.VMEM((g // 2, 2, t // 8, 8, 128), jnp.float32),
                pltpu.VMEM((NS + 1, 2, 2, 72, lora), jnp.float32),
                pltpu.VMEM((NS + 1, 2, 72, lora), jnp.float32),
                pltpu.VMEM((g + 1, nx, 2, 16, lora), jnp.bfloat16),
                pltpu.VMEM((g + 1, nx - 1, 2, 16, lora), jnp.bfloat16),
                pltpu.VMEM((g + 1, 2, 128), jnp.float32),
                pltpu.VMEM((g + 1, nx - 1, 2, 128), jnp.float32),
                pltpu.VMEM((4, 128, 8), jnp.float32),
                pltpu.SemaphoreType.DMA((nr,)),
                pltpu.SemaphoreType.DMA((g, 8)),
                pltpu.SemaphoreType.DMA((g, 8)),
                pltpu.SemaphoreType.DMA((g,)),
                pltpu.SemaphoreType.DMA((g,)),
                pltpu.SemaphoreType.DMA((g, nx - 1)),
                pltpu.SemaphoreType.DMA((g, nx - 1)),
                pltpu.SemaphoreType.DMA((g, nx - 1)),
                pltpu.SemaphoreType.DMA((g, nx - 1)),
            ],
            compiler_params=pltpu.CompilerParams(vmem_limit_bytes=67043328, collective_id=0, has_side_effects=True),
        )(lens, qn, ct)
        return o

    return jax.shard_map(local, mesh=mesh, in_specs=(P('dp', 'dcp', None), P('dp', None, 'dcp', None, None), P('dp')), out_specs=P('dp', 'dcp', None), check_vma=False)
```

```python
import functools
import jax
import jax.numpy as jnp
from jax import lax
from jax.experimental import pallas as pl
from jax.experimental.pallas import tpu as pltpu
from jax.sharding import PartitionSpec as P

ROPE = 64
QK_DIM = 192
SCALE = QK_DIM ** -0.5
LOG2E = 1.4426950408889634
KP = 640
TQ = 64
TV = 64
NS = 4
NU = 4
MESH = pl.DeviceIdType.MESH


def kernel(lens_hbm, qn_hbm, c_hbm, o_hbm, lens_ref, qn_ref, o_ref, ylo, yhi, q_ref, lm_ref, qall, qt, s0_ref, s1_ref, accs, arecv, part, precv, lses, lrecv, cols,
           isem, osem, csem, qs, qr, ss, sr, ps, pr, ls, lr):
    me = lax.axis_index('dcp')
    dp = lax.axis_index('dp')
    x, c = me // 2, lax.rem(me, 2)
    nx = 4
    n = 2 * nx
    nr, page, k, b = c_hbm.shape
    g = b // 16
    t = nr * page
    lora = k - ROPE
    bf = jnp.bfloat16
    f32 = jnp.float32

    def at(dx, same):
        xx = lax.rem(x + dx + nx, nx)
        return (dp, xx * 2 + (c if same else 1 - c))

    def slot(dx):
        return c * nx + lax.rem(x + dx + nx, nx)

    def fetch(r, y):
        return pltpu.make_async_copy(c_hbm.at[r], y.at[pl.ds(lax.rem(r, nr // 2) * page, page), 0:k], csem.at[r])

    qin = pltpu.make_async_copy(qn_hbm, qn_ref, isem.at[0])
    lin = pltpu.make_async_copy(lens_hbm, lens_ref, isem.at[1])
    qin.start()
    lin.start()
    for r in range(4):
        fetch(r, ylo).start()

    barrier = pltpu.get_barrier_semaphore()
    for dev in (at(1, True), at(-1, True), at(2, True), at(0, False)):
        pl.semaphore_signal(barrier, inc=1, device_id=dev, device_id_type=MESH)

    qin.wait()
    for kt in range(KP // 128):
        r0, r1 = kt * 128, min(kt * 128 + 128, k)
        hs = []
        for h in range(2):
            xq = qn_ref[h, r0:r1]
            if r1 - r0 < 128:
                xq = jnp.concatenate([xq, jnp.zeros((128 - (r1 - r0), b), bf)], 0)
            hs.append(xq.T.astype(f32).reshape(g, 2, 1, 8, 128))
        q_ref[:, :, :, r0:r0 + 128] = jnp.concatenate(hs, axis=2).reshape(g, 2, 16, 128).astype(bf)

    sub = lax.broadcasted_iota(jnp.int32, (8, 128), 0)
    lane8 = lax.rem(lax.broadcasted_iota(jnp.int32, (8, 128), 1), 8)
    diag = lane8 == sub
    turn = lax.rem(sub - lane8 + 8, 8)
    lin.wait()
    for r in range(4, nr):
        fetch(r, ylo if r < nr // 2 else yhi).start()
    for gi in range(g):
        for o in range(2):
            v = jnp.zeros((8, 128), jnp.int32)
            for i in range(8):
                v = jnp.where(lane8 == i, lens_ref[gi * 16 + o * 8 + i], v)
            lm_ref[gi, o] = v

    def load(r, y):
        for i in range(2):
            fetch(2 * r + i, y).wait()
        for p in range(2 * page):
            i = lax.rem(r, nr // 4) * 2 * page + p
            for kt in range(lora // 128):
                y[i, kt * 128:(kt + 1) * 128] = y[i, kt * 128:(kt + 1) * 128].T
            xr = y[i, lora:k]
            y[i, lora:KP] = jnp.concatenate([xr, jnp.zeros((KP - k, b), xr.dtype)], 0).T

    load(0, ylo)
    pl.semaphore_wait(barrier, 4)

    def rc(src, dst, s, r, dev):
        return pltpu.make_async_remote_copy(src_ref=src, dst_ref=dst, send_sem=s, recv_sem=r, device_id=dev, device_id_type=MESH)

    def qsend(gi, kind):
        dev = {0: at(1, True), 1: at(-1, True), 2: at(1, True), 3: at(-1, True), 4: at(0, False)}[kind]
        if kind <= 1:
            src, dst = q_ref.at[gi], qall.at[gi, slot(0)]
        elif kind <= 3:
            src = dst = qall.at[gi, slot(-1 if kind == 2 else 1), kind - 2]
        else:
            src = dst = qall.at[gi, pl.ds(c * nx, nx)]
        return rc(src, dst, qs.at[gi, kind], qr.at[gi, kind], dev)

    def qwait(gi, kind):
        if kind <= 1:
            ref = qall.at[gi, slot(-1 if kind == 0 else 1)]
        elif kind <= 3:
            ref = qall.at[gi, slot(2), kind - 2]
        else:
            ref = qall.at[gi, pl.ds((1 - c) * nx, nx)]
        rc(ref, ref, qs.at[gi, kind], qr.at[gi, kind], at(0, False)).wait_recv()

    AHEAD = 3

    def own(gi):
        for kind in range(2):
            qsend(gi, kind).start()

    for gi in range(AHEAD):
        own(gi)
    for gi in range(g):
        qall[gi, slot(0)] = q_ref[gi]

    def relay1(gi):
        qwait(gi, 0)
        qsend(gi, 2).start()
        qwait(gi, 1)
        qsend(gi, 3).start()

        @pl.when(gi + AHEAD < g)
        def _():
            own(gi + AHEAD)

    def relay2(gi):
        qwait(gi, 2)
        qwait(gi, 3)
        qsend(gi, 4).start()

    R1, R2 = 4, 8

    def relays(r):
        for rr, f in ((R1, relay1), (R2, relay2)):
            j = r - rr

            @pl.when((j >= 0) & (lax.rem(j + 30, 3) == 0) & (2 * (j // 3) < g))
            def _():
                f(2 * (j // 3))

            @pl.when((j >= 2) & (lax.rem(j + 28, 3) == 0) & (2 * ((j - 2) // 3) + 1 < g))
            def _():
                f(2 * ((j - 2) // 3) + 1)

    def count(rr):
        return len([gi for gi in range(g) if rr + (3 * gi + 1) // 2 < nr // 2])

    n1, n2 = count(R1), count(R2)

    def rows(ti, tn, gi, nk):
        y = ylo if ti < t // 2 else yhi
        ti = ti % (t // 2)
        parts = [y[pl.ds(ti, tn), pl.ds(kt * 128 + gi * 16, 16)].reshape(tn * 16, 128) for kt in range(nk)]
        return jnp.concatenate(parts, axis=1)

    def loadq(gi):
        qwait(gi, 4)
        reload(gi)

    def reload(gi):
        q0 = qall[gi, :, 0].reshape(128, KP)
        q1 = qall[gi, :, 1].reshape(128, KP)
        qt[...] = jnp.concatenate([q0, q1], axis=0).T

    def qk(gi, j, s_ref):
        s = jnp.dot(rows(j * TQ, TQ, gi, KP // 128), qt[...], preferred_element_type=jnp.float32)
        s = s.reshape(TQ // 8, 8, 2, 8, 256)
        blk = lax.broadcasted_iota(jnp.int32, (TQ // 8, 1, 1), 0) + j * (TQ // 8)
        pos = (blk * n + me) * page + turn[None]
        for o in range(2):
            d = s[:, 0, o, :, o * 128:(o + 1) * 128]
            for i in range(1, 8):
                d = jnp.where((turn == i)[None], pltpu.roll(s[:, i, o, :, o * 128:(o + 1) * 128], i, 1), d)
            d = jnp.where(pos < lm_ref[gi, o][None], d * (SCALE * LOG2E), -jnp.inf)
            s_ref[gi // 2, o, pl.ds(j * (TQ // 8), TQ // 8)] = d

    def qks(gi, j0, j1, s_ref):
        for j in range(j0, j1):
            qk(gi, j, s_ref)

    def fix(m):
        return jnp.where(m == -jnp.inf, 0.0, m)

    def maxes(gi, s_ref):
        return [jnp.max(jnp.max(s_ref[gi // 2, o], axis=0), axis=0, keepdims=True) for o in range(2)]

    lane = lax.broadcasted_iota(jnp.int32, (128, TV * 16), 1)
    first = lax.rem(lane, 16) < 8

    def pv(gi, j, s_ref, mf, l, acc):
        pe = []
        lo = []
        for o in range(2):
            p = jnp.exp2(s_ref[gi // 2, o, pl.ds(j * (TV // 8), TV // 8)] - mf[o][None])
            lo.append(l[o] + jnp.sum(p, axis=0))
            q = [p] + [pltpu.roll(p, 8 - i, 1) for i in range(1, 8)]
            q = jnp.stack([jnp.where(diag[None], a, 0.0) for a in q], axis=1)
            pe.append(q.reshape(TV, 8, 128))
        pm = jnp.concatenate(pe, axis=1).astype(bf).reshape(TV * 16, 128).T
        z = jnp.zeros_like(pm)
        pt = jnp.concatenate([jnp.where(first, pm, z), jnp.where(first, z, pm)], axis=0)
        acc = acc + jnp.dot(pt, rows(j * TV, TV, gi, lora // 128), preferred_element_type=jnp.float32)
        return tuple(lo), acc

    def asend(gi):
        return rc(accs.at[lax.rem(gi, NS), 1 - c], arecv.at[lax.rem(gi, NS)], ss.at[gi], sr.at[gi], at(0, False))

    def put(gi, m, l, acc):
        gs = lax.rem(gi, NS)

        @pl.when(gi >= NS)
        def _():
            asend(gi - NS).wait_send()

        for o in range(2):
            lo = jnp.sum(l[o], axis=0, keepdims=True)
            st = jnp.concatenate([m[o], lo, jnp.zeros((6, 128), jnp.float32)], axis=0)
            for h in range(2):
                r0 = o * 128 + h * 64
                accs[gs, h, o, 0:64] = acc[r0:r0 + 64]
                accs[gs, h, o, 64:72, 0:128] = st
        asend(gi).start()

    def psend(gi, dx):
        return rc(part.at[gi, lax.rem(x + dx, nx)], precv.at[gi, 3 - dx], ps.at[gi, dx - 1], pr.at[gi, 3 - dx], at(dx, True))

    def lsend(gi, dx):
        return rc(lses.at[gi], lrecv.at[gi, 3 - dx], ls.at[gi, dx - 1], lr.at[gi, 3 - dx], at(dx, True))

    def merge_wait(gi):
        asend(gi).wait_recv()

    def merge(gi, live=None):
        gs = lax.rem(gi, NS)
        if live is not None:
            gs, gi = lax.select(live, gs, NS), lax.select(live, gi, g)
        for o in range(2):
            m1, l1 = accs[gs, c, o, 64:65, 0:128], accs[gs, c, o, 65:66, 0:128]
            m2, l2 = arecv[gs, o, 64:65, 0:128], arecv[gs, o, 65:66, 0:128]
            mm = jnp.maximum(m1, m2)
            ms = fix(mm)
            w1, w2 = jnp.exp2(m1 - ms), jnp.exp2(m2 - ms)
            lt = w1 * l1 + w2 * l2
            has = lt > 0.0
            lsafe = jnp.where(has, lt, 1.0)
            lses[gi, o:o + 1] = jnp.where(has, ms + jnp.log2(lsafe), -jnp.inf)
            wr = jnp.concatenate([w1 / lsafe, w2 / lsafe, jnp.zeros((6, 128), f32)], axis=0)
            cols[o] = wr.T
            w = cols[o, pl.ds(c * 64, 64)]
            od = accs[gs, c, o, 0:64] * w[:, 0:1] + arecv[gs, o, 0:64] * w[:, 1:2]
            part[gi, :, o] = od.astype(bf).reshape(nx, 16, lora)

    def merge_send(gi):
        for dx in (2, 1, 3):
            psend(gi, dx).start()
            lsend(gi, dx).start()

    def final_wait(gi):
        for dx in range(1, 4):
            psend(gi, dx).wait_recv()
            lsend(gi, dx).wait_recv()

    def oput(gi):
        w = pl.ds(gi * 16, 16)
        return pltpu.make_async_copy(o_ref.at[w], o_hbm.at[w], osem.at[gi])

    def final(gi, live=None):
        og = gi
        if live is not None:
            og, gi = lax.select(live, gi, 0), lax.select(live, gi, g)
        for o in range(2):
            le = [lses[gi, o:o + 1]] + [lrecv[gi, i, o:o + 1] for i in range(3)]
            top = functools.reduce(jnp.maximum, le)
            w = [jnp.exp2(a - top) for a in le]
            tot = sum(w)
            wr = jnp.concatenate([a / tot for a in w] + [jnp.zeros((4, 128), f32)], axis=0)
            cols[2 + o] = wr.T
            wc = cols[2 + o, pl.ds(c * 64 + x * 16, 16)]
            od = part[gi, x, o].astype(f32) * wc[:, 0:1]
            for i in range(3):
                od = od + precv[gi, i, o].astype(f32) * wc[:, i + 1:i + 2]
            o_ref[pl.ds(og * 16 + o * 8, 8)] = jnp.stack([od[0:8], od[8:16]], axis=1).astype(bf)

    l0 = (jnp.zeros((8, 128), jnp.float32),) * 2
    a0 = jnp.zeros((256, lora), jnp.float32)

    LAG = 5
    ML = 2

    def top(ga):
        @pl.when(ga + n1 < g)
        def _():
            relay1(ga + n1)

        @pl.when(ga + n2 < g)
        def _():
            relay2(ga + n2)

        @pl.when(ga >= ML)
        def _():
            merge_wait(ga - ML)

        @pl.when(ga >= LAG)
        def _():
            final_wait(ga - LAG)

    def mid(ga):
        merge(lax.rem(ga - ML + NS * g, NS * g), ga >= ML)
        final(ga - LAG, ga >= LAG)

    def end(ga, m, l, acc):
        @pl.when(ga >= ML)
        def _():
            merge_send(ga - ML)

        @pl.when(ga >= LAG)
        def _():
            oput(ga - LAG).start()

        put(ga, m, l, acc)

    NJ = t // TQ

    def both(ga, sa, gb, sb, j0):
        top(ga)
        (reload if j0 else loadq)(gb)
        mid(ga)
        m = maxes(ga, sa)
        mf = [fix(a) for a in m]
        l, acc = l0, a0
        done = j0
        for j in range(NJ):
            todo = j0 + (NJ - j0) * (j + 1) // NJ
            qks(gb, done, todo, sb)
            done = todo
            l, acc = pv(ga, j, sa, mf, l, acc)
        end(ga, m, l, acc)

    def only_pv(gi, s_ref):
        top(gi)
        mid(gi)
        m = maxes(gi, s_ref)
        mf = [fix(a) for a in m]
        l, acc = l0, a0
        for j in range(NJ):
            l, acc = pv(gi, j, s_ref, mf, l, acc)
        end(gi, m, l, acc)

    def pair(i, _, j0):
        both(2 * i, s0_ref, 2 * i + 1, s1_ref, j0)
        both(2 * i + 1, s1_ref, 2 * i + 2, s0_ref, j0)
        return 0

    H = NJ // 2
    U0 = nr // 2 - NU

    def astep(r, _, y):
        relays(r)
        load(r, y)
        return 0

    def bstep(i, _):
        for s_ref, e in ((s0_ref, 0), (s1_ref, 1)):
            r = U0 + 2 * i + e
            relays(r)
            loadq(2 * i + e)
            load(r, yhi)
            qks(2 * i + e, 0, H, s_ref)
        return 0

    lax.fori_loop(1, nr // 4, functools.partial(astep, y=ylo), 0)
    lax.fori_loop(nr // 4, U0, functools.partial(astep, y=yhi), 0)
    lax.fori_loop(0, NU // 2, bstep, 0)
    reload(0)
    qks(0, H, NJ, s0_ref)
    lax.fori_loop(0, NU // 2 - 1, functools.partial(pair, j0=H), 0)
    both(jnp.int32(NU - 2), s0_ref, jnp.int32(NU - 1), s1_ref, H)
    both(jnp.int32(NU - 1), s1_ref, jnp.int32(NU), s0_ref, 0)
    lax.fori_loop(NU // 2, g // 2 - 1, functools.partial(pair, j0=0), 0)
    last = jnp.int32(g - 1)
    both(last - 1, s0_ref, last, s1_ref, 0)
    only_pv(last, s1_ref)
    for gi in range(g - ML, g - 1):
        merge_wait(gi)
        merge(gi)
        merge_send(gi)
    for gi in range(g - LAG, g - ML - 1):
        final_wait(gi)
        final(gi)
        oput(gi).start()
    merge_wait(g - 1)
    merge(g - 1)
    merge_send(g - 1)
    def drain(gi, _):
        for kind in range(5):
            qsend(gi, kind).wait_send()
        @pl.when(gi >= g - NS)
        def _():
            asend(gi).wait_send()

        for dx in range(1, 4):
            psend(gi, dx).wait_send()
            lsend(gi, dx).wait_send()
        return 0

    lax.fori_loop(0, g, drain, 0)

    for gi in range(g - ML - 1, g):
        final_wait(gi)
        final(gi)
        oput(gi).start()
    for gi in range(g):
        oput(gi).wait()


def solution(mesh):
    n = mesh.shape['dcp']
    nx = n // 2

    def local(q, cache, lens):
        b, hl, k = q.shape
        nr, page = cache.shape[1], cache.shape[3]
        lora = k - ROPE
        g = b // 16
        t = nr * page
        qn = jnp.transpose(q, (1, 2, 0))
        ct = jnp.transpose(cache, (1, 2, 3, 4, 0)).reshape(nr, page, k, b)
        o = pl.pallas_call(
            kernel,
            out_shape=jax.ShapeDtypeStruct((b, hl, lora), jnp.bfloat16),
            in_specs=[pl.BlockSpec(memory_space=pl.ANY)] * 3,
            out_specs=pl.BlockSpec(memory_space=pl.ANY),
            scratch_shapes=[
                pltpu.SMEM((b,), jnp.int32),
                pltpu.VMEM((hl, k, b), jnp.bfloat16),
                pltpu.VMEM((b, hl, lora), jnp.bfloat16),
                pltpu.VMEM((t // 2, KP, b), jnp.bfloat16),
                pltpu.VMEM((t // 2, KP, b), jnp.bfloat16),
                pltpu.VMEM((g, 2, 16, KP), jnp.bfloat16),
                pltpu.VMEM((g, 2, 8, 128), jnp.int32),
                pltpu.VMEM((g, n, 2, 16, KP), jnp.bfloat16),
                pltpu.VMEM((KP, 256), jnp.bfloat16),
                pltpu.VMEM((g // 2, 2, t // 8, 8, 128), jnp.float32),
                pltpu.VMEM((g // 2, 2, t // 8, 8, 128), jnp.float32),
                pltpu.VMEM((NS + 1, 2, 2, 72, lora), jnp.float32),
                pltpu.VMEM((NS + 1, 2, 72, lora), jnp.float32),
                pltpu.VMEM((g + 1, nx, 2, 16, lora), jnp.bfloat16),
                pltpu.VMEM((g + 1, nx - 1, 2, 16, lora), jnp.bfloat16),
                pltpu.VMEM((g + 1, 2, 128), jnp.float32),
                pltpu.VMEM((g + 1, nx - 1, 2, 128), jnp.float32),
                pltpu.VMEM((4, 128, 8), jnp.float32),
                pltpu.SemaphoreType.DMA((2,)),
                pltpu.SemaphoreType.DMA((g,)),
                pltpu.SemaphoreType.DMA((nr,)),
                pltpu.SemaphoreType.DMA((g, 5)),
                pltpu.SemaphoreType.DMA((g, 5)),
                pltpu.SemaphoreType.DMA((g,)),
                pltpu.SemaphoreType.DMA((g,)),
                pltpu.SemaphoreType.DMA((g, nx - 1)),
                pltpu.SemaphoreType.DMA((g, nx - 1)),
                pltpu.SemaphoreType.DMA((g, nx - 1)),
                pltpu.SemaphoreType.DMA((g, nx - 1)),
            ],
            compiler_params=pltpu.CompilerParams(vmem_limit_bytes=67043328, collective_id=0, has_side_effects=True),
        )(lens, qn, ct)
        return o

    return jax.shard_map(local, mesh=mesh, in_specs=(P('dp', 'dcp', None), P('dp', None, 'dcp', None, None), P('dp')), out_specs=P('dp', 'dcp', None), check_vma=False)
```

```python
import functools
import jax
import jax.numpy as jnp
from jax import lax
from jax.experimental import pallas as pl
from jax.experimental.pallas import tpu as pltpu
from jax.sharding import PartitionSpec as P

ROPE = 64
QK_DIM = 192
SCALE = QK_DIM ** -0.5
LOG2E = 1.4426950408889634
KP = 640
TQ = 64
TV = 64
NS = 4
NU = 4
MESH = pl.DeviceIdType.MESH


def kernel(lens_hbm, qn_hbm, c_hbm, o_hbm, lens_ref, qn_ref, o_ref, ylo, yhi, q_ref, lm_ref, qall, qt, s0_ref, s1_ref, accs, arecv, part, precv, lses, lrecv, cols,
           isem, osem, csem, qs, qr, ss, sr, ps, pr, ls, lr):
    me = lax.axis_index('dcp')
    dp = lax.axis_index('dp')
    x, c = me // 2, lax.rem(me, 2)
    nx = 4
    n = 2 * nx
    nr, page, k, b = c_hbm.shape
    g = b // 16
    t = nr * page
    lora = k - ROPE
    bf = jnp.bfloat16
    f32 = jnp.float32

    def at(dx, same):
        xx = lax.rem(x + dx + nx, nx)
        return (dp, xx * 2 + (c if same else 1 - c))

    def slot(dx):
        return c * nx + lax.rem(x + dx + nx, nx)

    def fetch(r, y):
        return pltpu.make_async_copy(c_hbm.at[r], y.at[pl.ds(lax.rem(r, nr // 2) * page, page), 0:k], csem.at[r])

    qin = pltpu.make_async_copy(qn_hbm, qn_ref, isem.at[0])
    lin = pltpu.make_async_copy(lens_hbm, lens_ref, isem.at[1])
    qin.start()
    lin.start()
    for r in range(4):
        fetch(r, ylo).start()

    barrier = pltpu.get_barrier_semaphore()
    for dev in (at(1, True), at(-1, True), at(2, True), at(0, False)):
        pl.semaphore_signal(barrier, inc=1, device_id=dev, device_id_type=MESH)

    qin.wait()
    for kt in range(KP // 128):
        r0, r1 = kt * 128, min(kt * 128 + 128, k)
        hs = []
        for h in range(2):
            xq = qn_ref[h, r0:r1]
            if r1 - r0 < 128:
                xq = jnp.concatenate([xq, jnp.zeros((128 - (r1 - r0), b), bf)], 0)
            hs.append(xq.T.astype(f32).reshape(g, 2, 1, 8, 128))
        q_ref[:, :, :, r0:r0 + 128] = jnp.concatenate(hs, axis=2).reshape(g, 2, 16, 128).astype(bf)

    sub = lax.broadcasted_iota(jnp.int32, (8, 128), 0)
    lane8 = lax.rem(lax.broadcasted_iota(jnp.int32, (8, 128), 1), 8)
    diag = lane8 == sub
    turn = lax.rem(sub - lane8 + 8, 8)
    lin.wait()
    for r in range(4, nr):
        fetch(r, ylo if r < nr // 2 else yhi).start()
    for gi in range(g):
        for o in range(2):
            v = jnp.zeros((8, 128), jnp.int32)
            for i in range(8):
                v = jnp.where(lane8 == i, lens_ref[gi * 16 + o * 8 + i], v)
            lm_ref[gi, o] = v

    def load(r, y):
        for i in range(2):
            fetch(2 * r + i, y).wait()
        for p in range(2 * page):
            i = lax.rem(r, nr // 4) * 2 * page + p
            for kt in range(lora // 128):
                y[i, kt * 128:(kt + 1) * 128] = y[i, kt * 128:(kt + 1) * 128].T
            xr = y[i, lora:k]
            y[i, lora:KP] = jnp.concatenate([xr, jnp.zeros((KP - k, b), xr.dtype)], 0).T

    load(0, ylo)
    pl.semaphore_wait(barrier, 4)

    def rc(src, dst, s, r, dev):
        return pltpu.make_async_remote_copy(src_ref=src, dst_ref=dst, send_sem=s, recv_sem=r, device_id=dev, device_id_type=MESH)

    def qsend(gi, kind):
        dev = {0: at(1, True), 1: at(-1, True), 2: at(1, True), 3: at(-1, True), 4: at(0, False)}[kind]
        if kind <= 1:
            src, dst = q_ref.at[gi], qall.at[gi, slot(0)]
        elif kind <= 3:
            src = dst = qall.at[gi, slot(-1 if kind == 2 else 1), kind - 2]
        else:
            src = dst = qall.at[gi, pl.ds(c * nx, nx)]
        return rc(src, dst, qs.at[gi, kind], qr.at[gi, kind], dev)

    def qwait(gi, kind):
        if kind <= 1:
            ref = qall.at[gi, slot(-1 if kind == 0 else 1)]
        elif kind <= 3:
            ref = qall.at[gi, slot(2), kind - 2]
        else:
            ref = qall.at[gi, pl.ds((1 - c) * nx, nx)]
        rc(ref, ref, qs.at[gi, kind], qr.at[gi, kind], at(0, False)).wait_recv()

    AHEAD = 4

    def own(gi):
        for kind in range(2):
            qsend(gi, kind).start()

    for gi in range(AHEAD):
        own(gi)
    for gi in range(g):
        qall[gi, slot(0)] = q_ref[gi]

    def relay1(gi):
        qwait(gi, 0)
        qsend(gi, 2).start()
        qwait(gi, 1)
        qsend(gi, 3).start()

        @pl.when(gi + AHEAD < g)
        def _():
            own(gi + AHEAD)

    def relay2(gi):
        qwait(gi, 2)
        qwait(gi, 3)
        qsend(gi, 4).start()

    R1, R2 = 4, 8

    def relays(r):
        for rr, f in ((R1, relay1), (R2, relay2)):
            j = r - rr

            @pl.when((j >= 0) & (lax.rem(j + 30, 3) == 0) & (2 * (j // 3) < g))
            def _():
                f(2 * (j // 3))

            @pl.when((j >= 2) & (lax.rem(j + 28, 3) == 0) & (2 * ((j - 2) // 3) + 1 < g))
            def _():
                f(2 * ((j - 2) // 3) + 1)

    def count(rr):
        return len([gi for gi in range(g) if rr + (3 * gi + 1) // 2 < nr // 2])

    n1, n2 = count(R1), count(R2)

    def rows(ti, tn, gi, nk):
        y = ylo if ti < t // 2 else yhi
        ti = ti % (t // 2)
        parts = [y[pl.ds(ti, tn), pl.ds(kt * 128 + gi * 16, 16)].reshape(tn * 16, 128) for kt in range(nk)]
        return jnp.concatenate(parts, axis=1)

    def loadq(gi):
        qwait(gi, 4)
        reload(gi)

    def reload(gi):
        q0 = qall[gi, :, 0].reshape(128, KP)
        q1 = qall[gi, :, 1].reshape(128, KP)
        qt[...] = jnp.concatenate([q0, q1], axis=0).T

    def qk(gi, j, s_ref):
        s = jnp.dot(rows(j * TQ, TQ, gi, KP // 128), qt[...], preferred_element_type=jnp.float32)
        s = s.reshape(TQ // 8, 8, 2, 8, 256)
        blk = lax.broadcasted_iota(jnp.int32, (TQ // 8, 1, 1), 0) + j * (TQ // 8)
        pos = (blk * n + me) * page + turn[None]
        for o in range(2):
            d = s[:, 0, o, :, o * 128:(o + 1) * 128]
            for i in range(1, 8):
                d = jnp.where((turn == i)[None], pltpu.roll(s[:, i, o, :, o * 128:(o + 1) * 128], i, 1), d)
            d = jnp.where(pos < lm_ref[gi, o][None], d * (SCALE * LOG2E), -jnp.inf)
            s_ref[gi // 2, o, pl.ds(j * (TQ // 8), TQ // 8)] = d

    def qks(gi, j0, j1, s_ref):
        for j in range(j0, j1):
            qk(gi, j, s_ref)

    def fix(m):
        return jnp.where(m == -jnp.inf, 0.0, m)

    def maxes(gi, s_ref):
        return [jnp.max(jnp.max(s_ref[gi // 2, o], axis=0), axis=0, keepdims=True) for o in range(2)]

    lane = lax.broadcasted_iota(jnp.int32, (128, TV * 16), 1)
    first = lax.rem(lane, 16) < 8

    def pv(gi, j, s_ref, mf, l, acc):
        pe = []
        lo = []
        for o in range(2):
            p = jnp.exp2(s_ref[gi // 2, o, pl.ds(j * (TV // 8), TV // 8)] - mf[o][None])
            lo.append(l[o] + jnp.sum(p, axis=0))
            q = [p] + [pltpu.roll(p, 8 - i, 1) for i in range(1, 8)]
            q = jnp.stack([jnp.where(diag[None], a, 0.0) for a in q], axis=1)
            pe.append(q.reshape(TV, 8, 128))
        pm = jnp.concatenate(pe, axis=1).astype(bf).reshape(TV * 16, 128).T
        z = jnp.zeros_like(pm)
        pt = jnp.concatenate([jnp.where(first, pm, z), jnp.where(first, z, pm)], axis=0)
        acc = acc + jnp.dot(pt, rows(j * TV, TV, gi, lora // 128), preferred_element_type=jnp.float32)
        return tuple(lo), acc

    def asend(gi):
        return rc(accs.at[lax.rem(gi, NS), 1 - c], arecv.at[lax.rem(gi, NS)], ss.at[gi], sr.at[gi], at(0, False))

    def put(gi, m, l, acc):
        gs = lax.rem(gi, NS)

        @pl.when(gi >= NS)
        def _():
            asend(gi - NS).wait_send()

        for o in range(2):
            lo = jnp.sum(l[o], axis=0, keepdims=True)
            st = jnp.concatenate([m[o], lo, jnp.zeros((6, 128), jnp.float32)], axis=0)
            for h in range(2):
                r0 = o * 128 + h * 64
                accs[gs, h, o, 0:64] = acc[r0:r0 + 64]
                accs[gs, h, o, 64:72, 0:128] = st
        asend(gi).start()

    def psend(gi, dx):
        return rc(part.at[gi, lax.rem(x + dx, nx)], precv.at[gi, 3 - dx], ps.at[gi, dx - 1], pr.at[gi, 3 - dx], at(dx, True))

    def lsend(gi, dx):
        return rc(lses.at[gi], lrecv.at[gi, 3 - dx], ls.at[gi, dx - 1], lr.at[gi, 3 - dx], at(dx, True))

    def merge_wait(gi):
        asend(gi).wait_recv()

    def merge(gi, live=None):
        gs = lax.rem(gi, NS)
        if live is not None:
            gs, gi = lax.select(live, gs, NS), lax.select(live, gi, g)
        for o in range(2):
            m1, l1 = accs[gs, c, o, 64:65, 0:128], accs[gs, c, o, 65:66, 0:128]
            m2, l2 = arecv[gs, o, 64:65, 0:128], arecv[gs, o, 65:66, 0:128]
            mm = jnp.maximum(m1, m2)
            ms = fix(mm)
            w1, w2 = jnp.exp2(m1 - ms), jnp.exp2(m2 - ms)
            lt = w1 * l1 + w2 * l2
            has = lt > 0.0
            lsafe = jnp.where(has, lt, 1.0)
            lses[gi, o:o + 1] = jnp.where(has, ms + jnp.log2(lsafe), -jnp.inf)
            wr = jnp.concatenate([w1 / lsafe, w2 / lsafe, jnp.zeros((6, 128), f32)], axis=0)
            cols[o] = wr.T
            w = cols[o, pl.ds(c * 64, 64)]
            od = accs[gs, c, o, 0:64] * w[:, 0:1] + arecv[gs, o, 0:64] * w[:, 1:2]
            part[gi, :, o] = od.astype(bf).reshape(nx, 16, lora)

    def merge_send(gi):
        for dx in (2, 1, 3):
            psend(gi, dx).start()
            lsend(gi, dx).start()

    def final_wait(gi):
        for dx in range(1, 4):
            psend(gi, dx).wait_recv()
            lsend(gi, dx).wait_recv()

    def oput(gi):
        w = pl.ds(gi * 16, 16)
        return pltpu.make_async_copy(o_ref.at[w], o_hbm.at[w], osem.at[gi])

    def final(gi, live=None):
        og = gi
        if live is not None:
            og, gi = lax.select(live, gi, 0), lax.select(live, gi, g)
        for o in range(2):
            le = [lses[gi, o:o + 1]] + [lrecv[gi, i, o:o + 1] for i in range(3)]
            top = functools.reduce(jnp.maximum, le)
            w = [jnp.exp2(a - top) for a in le]
            tot = sum(w)
            wr = jnp.concatenate([a / tot for a in w] + [jnp.zeros((4, 128), f32)], axis=0)
            cols[2 + o] = wr.T
            wc = cols[2 + o, pl.ds(c * 64 + x * 16, 16)]
            od = part[gi, x, o].astype(f32) * wc[:, 0:1]
            for i in range(3):
                od = od + precv[gi, i, o].astype(f32) * wc[:, i + 1:i + 2]
            o_ref[pl.ds(og * 16 + o * 8, 8)] = jnp.stack([od[0:8], od[8:16]], axis=1).astype(bf)

    l0 = (jnp.zeros((8, 128), jnp.float32),) * 2
    a0 = jnp.zeros((256, lora), jnp.float32)

    LAG = 5
    ML = 2

    def top(ga):
        @pl.when(ga + n1 < g)
        def _():
            relay1(ga + n1)

        @pl.when(ga + n2 < g)
        def _():
            relay2(ga + n2)

        @pl.when(ga >= ML)
        def _():
            merge_wait(ga - ML)

        @pl.when(ga >= LAG)
        def _():
            final_wait(ga - LAG)

    def mid(ga):
        merge(lax.rem(ga - ML + NS * g, NS * g), ga >= ML)
        final(ga - LAG, ga >= LAG)

    def end(ga, m, l, acc):
        @pl.when(ga >= ML)
        def _():
            merge_send(ga - ML)

        @pl.when(ga >= LAG)
        def _():
            oput(ga - LAG).start()

        put(ga, m, l, acc)

    NJ = t // TQ

    def both(ga, sa, gb, sb, j0):
        top(ga)
        (reload if j0 else loadq)(gb)
        mid(ga)
        m = maxes(ga, sa)
        mf = [fix(a) for a in m]
        l, acc = l0, a0
        done = j0
        for j in range(NJ):
            todo = j0 + (NJ - j0) * (j + 1) // NJ
            qks(gb, done, todo, sb)
            done = todo
            l, acc = pv(ga, j, sa, mf, l, acc)
        end(ga, m, l, acc)

    def only_pv(gi, s_ref):
        top(gi)
        mid(gi)
        merge_send(gi - ML)
        oput(gi - LAG).start()
        m = maxes(gi, s_ref)
        mf = [fix(a) for a in m]
        l, acc = l0, a0
        for j in range(NJ):
            if j == NJ // 2:
                merge_wait(gi - 1)
                merge(gi - 1)
                merge_send(gi - 1)
            l, acc = pv(gi, j, s_ref, mf, l, acc)
        put(gi, m, l, acc)

    def pair(i, _, j0):
        both(2 * i, s0_ref, 2 * i + 1, s1_ref, j0)
        both(2 * i + 1, s1_ref, 2 * i + 2, s0_ref, j0)
        return 0

    H = NJ // 2
    U0 = nr // 2 - NU

    def astep(r, _, y):
        relays(r)
        load(r, y)
        return 0

    def bstep(i, _):
        for s_ref, e in ((s0_ref, 0), (s1_ref, 1)):
            r = U0 + 2 * i + e
            relays(r)
            loadq(2 * i + e)
            load(r, yhi)
            qks(2 * i + e, 0, H, s_ref)
        return 0

    lax.fori_loop(1, nr // 4, functools.partial(astep, y=ylo), 0)
    lax.fori_loop(nr // 4, U0, functools.partial(astep, y=yhi), 0)
    lax.fori_loop(0, NU // 2, bstep, 0)
    reload(0)
    qks(0, H, NJ, s0_ref)
    lax.fori_loop(0, NU // 2 - 1, functools.partial(pair, j0=H), 0)
    both(jnp.int32(NU - 2), s0_ref, jnp.int32(NU - 1), s1_ref, H)
    both(jnp.int32(NU - 1), s1_ref, jnp.int32(NU), s0_ref, 0)
    lax.fori_loop(NU // 2, g // 2 - 1, functools.partial(pair, j0=0), 0)
    last = jnp.int32(g - 1)
    both(last - 1, s0_ref, last, s1_ref, 0)
    only_pv(last, s1_ref)
    for gi in range(g - LAG, g - ML - 1):
        final_wait(gi)
        final(gi)
        oput(gi).start()
    merge_wait(g - 1)
    merge(g - 1)
    merge_send(g - 1)
    def drain(gi, _):
        for kind in range(5):
            qsend(gi, kind).wait_send()
        @pl.when(gi >= g - NS)
        def _():
            asend(gi).wait_send()

        for dx in range(1, 4):
            psend(gi, dx).wait_send()
            lsend(gi, dx).wait_send()
        return 0

    lax.fori_loop(0, g, drain, 0)

    for gi in range(g - ML - 1, g):
        final_wait(gi)
        final(gi)
        oput(gi).start()
    for gi in range(g):
        oput(gi).wait()


def solution(mesh):
    n = mesh.shape['dcp']
    nx = n // 2

    def local(q, cache, lens):
        b, hl, k = q.shape
        nr, page = cache.shape[1], cache.shape[3]
        lora = k - ROPE
        g = b // 16
        t = nr * page
        qn = jnp.transpose(q, (1, 2, 0))
        ct = jnp.transpose(cache, (1, 2, 3, 4, 0)).reshape(nr, page, k, b)
        o = pl.pallas_call(
            kernel,
            out_shape=jax.ShapeDtypeStruct((b, hl, lora), jnp.bfloat16),
            in_specs=[pl.BlockSpec(memory_space=pl.ANY)] * 3,
            out_specs=pl.BlockSpec(memory_space=pl.ANY),
            scratch_shapes=[
                pltpu.SMEM((b,), jnp.int32),
                pltpu.VMEM((hl, k, b), jnp.bfloat16),
                pltpu.VMEM((b, hl, lora), jnp.bfloat16),
                pltpu.VMEM((t // 2, KP, b), jnp.bfloat16),
                pltpu.VMEM((t // 2, KP, b), jnp.bfloat16),
                pltpu.VMEM((g, 2, 16, KP), jnp.bfloat16),
                pltpu.VMEM((g, 2, 8, 128), jnp.int32),
                pltpu.VMEM((g, n, 2, 16, KP), jnp.bfloat16),
                pltpu.VMEM((KP, 256), jnp.bfloat16),
                pltpu.VMEM((g // 2, 2, t // 8, 8, 128), jnp.float32),
                pltpu.VMEM((g // 2, 2, t // 8, 8, 128), jnp.float32),
                pltpu.VMEM((NS + 1, 2, 2, 72, lora), jnp.float32),
                pltpu.VMEM((NS + 1, 2, 72, lora), jnp.float32),
                pltpu.VMEM((g + 1, nx, 2, 16, lora), jnp.bfloat16),
                pltpu.VMEM((g + 1, nx - 1, 2, 16, lora), jnp.bfloat16),
                pltpu.VMEM((g + 1, 2, 128), jnp.float32),
                pltpu.VMEM((g + 1, nx - 1, 2, 128), jnp.float32),
                pltpu.VMEM((4, 128, 8), jnp.float32),
                pltpu.SemaphoreType.DMA((2,)),
                pltpu.SemaphoreType.DMA((g,)),
                pltpu.SemaphoreType.DMA((nr,)),
                pltpu.SemaphoreType.DMA((g, 5)),
                pltpu.SemaphoreType.DMA((g, 5)),
                pltpu.SemaphoreType.DMA((g,)),
                pltpu.SemaphoreType.DMA((g,)),
                pltpu.SemaphoreType.DMA((g, nx - 1)),
                pltpu.SemaphoreType.DMA((g, nx - 1)),
                pltpu.SemaphoreType.DMA((g, nx - 1)),
                pltpu.SemaphoreType.DMA((g, nx - 1)),
            ],
            compiler_params=pltpu.CompilerParams(vmem_limit_bytes=67043328, collective_id=0, has_side_effects=True),
        )(lens, qn, ct)
        return o

    return jax.shard_map(local, mesh=mesh, in_specs=(P('dp', 'dcp', None), P('dp', None, 'dcp', None, None), P('dp')), out_specs=P('dp', 'dcp', None), check_vma=False)
```
